32 devices in a mesh: pq: 8 (over z, x), hh: 4 (over y, core).
Axes of the slice: x: 2, y: 2, z: 4, core: 2. Of those that a mesh axis runs over, the one named last changes fastest.
Arguments:
- amplitudes: bfloat16 [4096, 2048], P('hh', 'pq'), may hold values from -6 to 6
- integrals: bfloat16 [4096, 2048], P('hh', 'pq'), may hold values from -0.001953125 to 0.001953125
- left_amps: bfloat16 [8, 4096, 1024], P(None, 'hh', 'pq'), may hold values from -6 to 6
Outputs:
- sigma_ladder: bfloat16 [8, 4096, 1024], P(None, 'hh', 'pq')
- subspace: float32 [8, 8], replicated
The draws below stay inside these ranges and needn't reach their ends.
All inputs are finite; a program needn't handle non-finite values.
Results may differ from the reference program's by a relative error of at most 0.0049.
Values may be sent and summed in bfloat16 or wider, within the bound.
No kernel may reach another device: no remote copies, remote signals or barrier semaphores. Data moves between devices by JAX's collectives and lax.ppermute only.
A program may use at most 64 MiB of HBM per device.

```python
import math
import jax
import jax.numpy as jnp
from jax import lax

OCC_PAIRS = 4096
ROOTS = 8
CD_PAIRS = 2048
AB_PAIRS = 1024


def levels(stream_key, extent, shards, smallest, largest):
    def one(dim, blocks):
        steps = jax.random.uniform(jax.random.fold_in(jax.random.fold_in(stream_key, 6), dim), (blocks,), jnp.float32, smallest / len(shards), largest / len(shards))
        return jnp.repeat(jnp.exp(steps), extent[dim] // blocks).reshape((-1,) + (1,) * (len(extent) - dim - 1))

    level = one(*shards[0])
    for cut in shards[1:]:
        level = level * one(*cut)
    return level


def centred(rng, shape, scale, bound, pieces=(), kind=jnp.bfloat16):
    entries = jax.random.normal(rng, shape, jnp.float32) * scale
    if len(pieces) > 0:
        entries = levels(rng, shape, pieces, -0.22, 0.18) * entries
    return jnp.clip(entries, min=-bound, max=bound).astype(kind)


def setup_inputs(seed: int = 0) -> dict:
    seeds = jax.random.split(jax.random.key(seed), 4)
    amplitudes = centred(seeds[0], (OCC_PAIRS, CD_PAIRS), 1.0, 6.0, ((0, 4), (1, 8)))
    integrals = centred(seeds[1], (OCC_PAIRS, CD_PAIRS), (CD_PAIRS * OCC_PAIRS) ** -0.5, 0.001953125, ((0, 4), (1, 8)))
    left_amps = centred(seeds[2], (ROOTS, OCC_PAIRS, AB_PAIRS), 1.0, 6.0, ((1, 4), (2, 8)))
    return dict(amplitudes=amplitudes, integrals=integrals, left_amps=left_amps)


def reference(amplitudes, integrals, left_amps):
    ladder = jnp.dot(amplitudes, integrals.T, preferred_element_type=jnp.float32).astype(jnp.bfloat16)
    ladder_trans = ladder.T

    def one_root(left_root):
        return jnp.dot(ladder_trans, left_root, preferred_element_type=jnp.float32).astype(jnp.bfloat16)
    sigma_ladder = lax.map(one_root, left_amps)
    flat_left = left_amps.reshape(ROOTS, -1)
    flat_sigma = sigma_ladder.reshape(ROOTS, -1)
    gram = jnp.dot(flat_left, flat_sigma.T, preferred_element_type=jnp.float32)
    subspace = gram * (1.0 / math.sqrt(OCC_PAIRS * AB_PAIRS))
    return (sigma_ladder, subspace)
```

```python
import math

import jax
import jax.numpy as jnp
from jax import lax
from jax.sharding import PartitionSpec as P

OCC_PAIRS = 4096
CORES = 2


def flip(x, axis, bits):
    n = lax.axis_size(axis)
    return lax.ppermute(x, axis, [(i, i ^ bits) for i in range(n)])


def tree_sum(parts):
    while len(parts) > 1:
        parts = [parts[i] + parts[i + 1] for i in range(0, len(parts), 2)]
    return parts[0]


def axis_sum(x, axis):
    n = lax.axis_size(axis)
    low = 1
    while low < n:
        span = min(8, n // low)
        x = tree_sum([x] + [flip(x, axis, k * low) for k in range(1, span)])
        low *= span
    return x


def x_shift(x, nx, s):
    n = lax.axis_size("pq")
    perm = [(i, i // nx * nx + (i + s) % nx) for i in range(n)]
    return lax.ppermute(x, "pq", perm)


def z_shift(x, nx):
    n = lax.axis_size("pq")
    return lax.ppermute(x, "pq", [(i, (i + nx) % n) for i in range(n)])


def gather_groups(block, nx):
    nz = lax.axis_size("pq") // nx
    groups = []
    for k in range(nz):
        if k > 0:
            block = z_shift(block, nx)
        group = [block]
        for s in range(1, nx):
            if k == 1 and s == 1:
                cut = block.shape[0] // 2
                moved = jnp.concatenate(
                    [
                        x_shift(block[:cut], nx, s),
                        z_shift(groups[0][1][cut:], nx),
                    ],
                    axis=0,
                )
            else:
                moved = x_shift(block, nx, s)
            group.append(moved)
        groups.append(group)
    return groups


def split(x):
    high = lax.reduce_precision(x, 8, 7)
    return high.astype(jnp.bfloat16), (x - high).astype(jnp.bfloat16)


def body(amplitudes, integrals, left_amps):
    roots, _, ab_cols = left_amps.shape
    cd_cols = integrals.shape[1]
    pq = lax.axis_size("pq")
    hh = lax.axis_size("hh")
    ny = hh // CORES
    nx = ny if pq % ny == 0 else 1
    half = cd_cols // CORES
    core = lax.axis_index("hh") % CORES

    def mine(x):
        return lax.dynamic_slice_in_dim(x, core * half, half, 1)

    def other(x):
        return lax.dynamic_slice_in_dim(x, (1 - core) * half, half, 1)

    amps_t = jnp.concatenate(
        [mine(amplitudes).T, flip(other(amplitudes).T, "hh", 1)], axis=1
    )
    left_both = jnp.concatenate([left_amps, flip(left_amps, "hh", 1)], axis=1)
    ints_t = jnp.concatenate([mine(integrals).T, other(integrals).T], axis=0)

    amp_groups = gather_groups(amps_t, nx)
    ints_t, _ = lax.optimization_barrier((ints_t, amp_groups[-1][0]))
    int_groups = gather_groups(ints_t, nx)

    rows_out = None
    for amp_group, int_group in zip(amp_groups, int_groups):
        part = lax.dot_general(
            jnp.concatenate(amp_group, axis=0),
            left_both,
            (((1,), (1,)), ((), ())),
            preferred_element_type=jnp.float32,
        )
        wire = part.astype(jnp.bfloat16)
        total = part
        for s in range(1, ny):
            perm = [
                (y * CORES + c, ((y + s) % ny) * CORES + c)
                for y in range(ny)
                for c in range(CORES)
            ]
            total = total + lax.ppermute(wire, "hh", perm).astype(jnp.float32)
        ints = jnp.concatenate(int_group, axis=0)
        for x in split(total):
            pair = (x, flip(x, "hh", 1))
            rows = jnp.concatenate(
                [
                    p[i * half : (i + 1) * half]
                    for i in range(nx)
                    for p in pair
                ],
                axis=0,
            )
            term = lax.dot_general(
                ints,
                rows,
                (((0,), (0,)), ((), ())),
                preferred_element_type=jnp.float32,
            )
            rows_out = term if rows_out is None else rows_out + term
    rows_out = jnp.transpose(rows_out, (1, 0, 2))
    sigma_out, rest = split(rows_out)
    flat_left = left_amps.reshape(roots, -1)
    local_gram = sum(
        jnp.dot(
            flat_left,
            s.reshape(roots, -1).T,
            preferred_element_type=jnp.float32,
        )
        for s in (sigma_out, rest)
    )
    factor = 1.0 / math.sqrt(OCC_PAIRS * ab_cols * pq)
    subspace = axis_sum(axis_sum(local_gram, "hh"), "pq") * factor
    return (sigma_out, subspace)


def solution(mesh):
    return jax.shard_map(
        body,
        mesh=mesh,
        in_specs=(P("hh", "pq"), P("hh", "pq"), P(None, "hh", "pq")),
        out_specs=(P(None, "hh", "pq"), P()),
        check_vma=False,
    )
```

```python
import math

import jax
import jax.numpy as jnp
from jax import lax
from jax.sharding import PartitionSpec as P

OCC_PAIRS = 4096
CORES = 2


def flip(x, axis, bits):
    n = lax.axis_size(axis)
    return lax.ppermute(x, axis, [(i, i ^ bits) for i in range(n)])


def tree_sum(parts):
    while len(parts) > 1:
        parts = [parts[i] + parts[i + 1] for i in range(0, len(parts), 2)]
    return parts[0]


def axis_sum(x, axis):
    n = lax.axis_size(axis)
    low = 1
    while low < n:
        span = min(4 if n <= 4 else 2, n // low)
        x = tree_sum([x] + [flip(x, axis, k * low) for k in range(1, span)])
        low *= span
    return x


def x_shift(x, nx, s):
    n = lax.axis_size("pq")
    perm = [(i, i // nx * nx + (i + s) % nx) for i in range(n)]
    return lax.ppermute(x, "pq", perm)


def z_shift(x, nx):
    n = lax.axis_size("pq")
    return lax.ppermute(x, "pq", [(i, (i + nx) % n) for i in range(n)])


def ring_rounds(block, nx, extra, tail):
    nz = lax.axis_size("pq") // nx
    groups = []
    for k in range(nz - 1):
        ahead = z_shift(block, nx)
        group = [block] + [x_shift(block, nx, s) for s in range(1, nx)]
        last = extra if k == nz - 2 else None
        ahead, group, last, tail_done = lax.optimization_barrier(
            (ahead, group, last, tail)
        )
        if k == 0:
            tail_out = tail_done
        tail = None
        groups.append(group)
        block = ahead
    group = [block]
    for s in range(1, nx):
        if s == 1:
            cut = block.shape[0] // 2
            group.append(
                (
                    x_shift(block[:cut], nx, s),
                    z_shift(groups[-1][1][cut:], nx),
                )
            )
        else:
            group.append(x_shift(block, nx, s))
    return groups, group, last, tail_out


def joined(group):
    parts = []
    for g in group:
        parts.extend(g if isinstance(g, (tuple, list)) else [g])
    return jnp.concatenate(parts, axis=0)


def split(x):
    high = lax.reduce_precision(x, 8, 7)
    return high.astype(jnp.bfloat16), (x - high).astype(jnp.bfloat16)


def body(amplitudes, integrals, left_amps):
    roots, _, ab_cols = left_amps.shape
    cd_cols = integrals.shape[1]
    pq = lax.axis_size("pq")
    hh = lax.axis_size("hh")
    ny = hh // CORES
    nx = ny if pq % ny == 0 else 1
    half = cd_cols // CORES
    core = lax.axis_index("hh") % CORES

    def mine(x):
        return lax.dynamic_slice_in_dim(x, core * half, half, 1)

    def other(x):
        return lax.dynamic_slice_in_dim(x, (1 - core) * half, half, 1)

    amps_t = jnp.concatenate(
        [mine(amplitudes).T, flip(other(amplitudes).T, "hh", 1)], axis=1
    )
    left_both = jnp.concatenate([left_amps, flip(left_amps, "hh", 1)], axis=1)
    ints_t = jnp.concatenate([mine(integrals).T, other(integrals).T], axis=0)

    amp_groups, amp_last, ints_t, _ = ring_rounds(amps_t, nx, ints_t, None)
    int_groups, int_last, _, amp_last = ring_rounds(ints_t, nx, None, amp_last)
    amp_groups.append(amp_last)
    int_groups.append(int_last)

    rows_out = None
    for amp_group, int_group in zip(amp_groups, int_groups):
        part = lax.dot_general(
            joined(amp_group),
            left_both,
            (((1,), (1,)), ((), ())),
            preferred_element_type=jnp.float32,
        )
        wire = part.astype(jnp.bfloat16)
        total = part
        for s in range(1, ny):
            perm = [
                (y * CORES + c, ((y + s) % ny) * CORES + c)
                for y in range(ny)
                for c in range(CORES)
            ]
            total = total + lax.ppermute(wire, "hh", perm).astype(jnp.float32)
        ints = joined(int_group)
        for x in split(total):
            pair = (x, flip(x, "hh", 1))
            rows = jnp.concatenate(
                [
                    p[i * half : (i + 1) * half]
                    for i in range(nx)
                    for p in pair
                ],
                axis=0,
            )
            term = lax.dot_general(
                ints,
                rows,
                (((0,), (0,)), ((), ())),
                preferred_element_type=jnp.float32,
            )
            rows_out = term if rows_out is None else rows_out + term
        rows_out = lax.optimization_barrier(rows_out)
    rows_out = jnp.transpose(rows_out, (1, 0, 2))
    sigma_out, rest = split(rows_out)
    flat_left = left_amps.reshape(roots, -1)
    local_gram = sum(
        jnp.dot(
            flat_left,
            s.reshape(roots, -1).T,
            preferred_element_type=jnp.float32,
        )
        for s in (sigma_out, rest)
    )
    factor = 1.0 / math.sqrt(OCC_PAIRS * ab_cols * pq)
    subspace = axis_sum(axis_sum(local_gram, "hh"), "pq") * factor
    return (sigma_out, subspace)


def solution(mesh):
    return jax.shard_map(
        body,
        mesh=mesh,
        in_specs=(P("hh", "pq"), P("hh", "pq"), P(None, "hh", "pq")),
        out_specs=(P(None, "hh", "pq"), P()),
        check_vma=False,
    )
```
